32 devices in a mesh: gz: 8 (over z, x), gy: 4 (over y, core).
Axes of the slice: x: 2, y: 2, z: 4, core: 2. Of those that a mesh axis runs over, the one named last changes fastest.
Arguments:
- populations: float32 [19, 24, 192, 128], P(None, 'gz', 'gy'), may hold values from 0.1 to 25, as said below
- solute: float32 [7, 24, 192, 128], P(None, 'gz', 'gy'), may hold values from 0.05 to 3, as said below
- pore_mask: int32 [24, 192, 128], P('gz', 'gy'), may hold values from 0 to 2
- mineral_ids: int32 [24, 192, 128], P('gz', 'gy'), may hold values from 0 to 7
- reaction_rates: float32 [8], replicated, may hold values from 0.05 to 0.6
- saturation: float32 [8], replicated, may hold values from 0.5 to 6
Outputs:
- flow_next: float32 [19, 24, 192, 128], P(None, 'gz', 'gy')
- solute_next: float32 [7, 24, 192, 128], P(None, 'gz', 'gy')
The draws below stay inside these ranges and needn't reach their ends.
Inputs may be any that keep to these rules, and one draw needn't show every extreme that they name: `populations`: every population is positive. `solute`: every population is positive.
All inputs are finite; a program needn't handle non-finite values.
Results may differ from the reference program's by a relative error of at most 0.0003.
Values sent between devices are 32-bit elements; how exact they have to be, the bound alone decides.
A program may use at most 64 MiB of HBM per device.

```python
import math
import jax
import jax.numpy as jnp
import numpy as np
from jax import lax

NX = 128
MINERALS = 8
NZ = 24
NY = 192


LINKS19 = np.array([[0, 0, 0], [1, 0, 0], [-1, 0, 0], [0, 1, 0], [0, -1, 0], [0, 0, 1], [0, 0, -1], [1, 1, 0], [-1, -1, 0], [1, -1, 0], [-1, 1, 0], [1, 0, 1], [-1, 0, -1], [1, 0, -1], [-1, 0, 1], [0, 1, 1], [0, -1, -1], [0, 1, -1], [0, -1, 1]])


WEIGHTS19 = np.array([1.0 / 3.0] + [1.0 / 18.0] * 6 + [1.0 / 36.0] * 12)


WEIGHTS7 = np.array([0.25] + [0.125] * 6)


def draw_populations(key, part):
    key_density, key_velocity, key_jitter = jax.random.split(jax.random.fold_in(key, 11), 3)
    grid_shape = (NZ, NY, NX)
    density_cell = 36.0 * jax.random.uniform(key_density, grid_shape, jnp.float32, 0.8, 1.2)
    velocity_cell = 0.025 * jnp.clip(jax.random.normal(key_velocity, (3,) + grid_shape, jnp.float32), -2.0, 2.0)
    jitter = 0.15 * jnp.clip(jax.random.normal(key_jitter, (19,) + grid_shape, jnp.float32), -2.0, 2.0)
    link_table = jnp.asarray(LINKS19, jnp.float32)
    projected = jnp.tensordot(link_table, velocity_cell, axes=1)
    speed = jnp.sum(velocity_cell * velocity_cell, 0)
    scaled = jnp.asarray(WEIGHTS19, jnp.float32)[:, None, None, None]
    balanced = scaled * density_cell * (1.0 + 3.0 * projected + 4.5 * projected * projected - 1.5 * speed)
    return (balanced * (1.0 + jitter)).astype(jnp.float32)


def draw_solute(key, part):
    key_level, key_jitter = jax.random.split(jax.random.fold_in(key, 23), 2)
    grid_shape = (NZ, NY, NX)
    concentration = jnp.exp(jax.random.uniform(key_level, grid_shape, jnp.float32, 0.0, 2.0794))
    jitter = 0.15 * jnp.clip(jax.random.normal(key_jitter, (7,) + grid_shape, jnp.float32), -2.0, 2.0)
    scaled = jnp.asarray(WEIGHTS7, jnp.float32)[:, None, None, None]
    return (scaled * concentration * (1.0 + jitter)).astype(jnp.float32)


def set_ends(drawn, own_key, least, largest):
    dims = drawn.shape
    index_at = [jax.random.randint(jax.random.fold_in(own_key, axis), (), 0, dims[axis]) for axis in range(len(dims))]
    drawn = drawn.at[tuple(index_at)].set(least)
    longest = dims.index(max(dims))
    index_at[longest] = (index_at[longest] + 1) % dims[longest]
    return drawn.at[tuple(index_at)].set(largest)


def setup_inputs(seed: int = 0) -> dict:
    key_of = jax.random.split(jax.random.key(seed), 7)
    populations = draw_populations(jax.random.fold_in(key_of[6], 71), 0)
    solute = draw_solute(jax.random.fold_in(key_of[6], 71), 0)
    pore_mask = set_ends(jax.random.randint(key_of[2], (NZ, NY, NX), 0, 3), jax.random.fold_in(key_of[2], 1), 0, 2).astype(jnp.int32)
    mineral_ids = set_ends(jax.random.randint(key_of[3], (NZ, NY, NX), 0, MINERALS), jax.random.fold_in(key_of[3], 1), 0, MINERALS - 1).astype(jnp.int32)
    reaction_rates = jnp.clip(jnp.exp(jax.random.uniform(key_of[4], (MINERALS,), jnp.float32, math.log(0.05), math.log(0.6))), 0.05, 0.6)
    saturation = jnp.clip(jax.random.uniform(key_of[5], (MINERALS,), jnp.float32, 0.5, 6.0), 0.5, 6.0)
    return {"populations": populations, "solute": solute, "pore_mask": pore_mask, "mineral_ids": mineral_ids, "reaction_rates": reaction_rates, "saturation": saturation}


LINKS19 = np.array([[0, 0, 0], [1, 0, 0], [-1, 0, 0], [0, 1, 0], [0, -1, 0], [0, 0, 1], [0, 0, -1], [1, 1, 0], [-1, -1, 0], [1, -1, 0], [-1, 1, 0], [1, 0, 1], [-1, 0, -1], [1, 0, -1], [-1, 0, 1], [0, 1, 1], [0, -1, -1], [0, 1, -1], [0, -1, 1]])
REVERSE19 = [0, 2, 1, 4, 3, 6, 5, 8, 7, 10, 9, 12, 11, 14, 13, 16, 15, 18, 17]
WEIGHTS19 = np.array([1.0 / 3.0] + [1.0 / 18.0] * 6 + [1.0 / 36.0] * 12)
WEIGHTS7 = np.array([0.25] + [0.125] * 6)
RELAX_FLOW = 1.25
RELAX_SOLUTE = 1.4


def moment(values, lattice):
    link_table = jnp.asarray(lattice, jnp.float32)
    return jnp.tensordot(link_table.T, values, axes=1, precision=lax.Precision.HIGHEST)


def equilibrium(density, velocity, lattice, weights, linear, quadratic, square_term):
    link_table = jnp.asarray(lattice, jnp.float32)
    projected = jnp.tensordot(link_table, velocity, axes=1, precision=lax.Precision.HIGHEST)
    speed = jnp.sum(velocity * velocity, 0)
    scaled = jnp.asarray(weights, jnp.float32)[:, None, None, None]
    return scaled * density * (1.0 + linear * projected + quadratic * projected * projected - square_term * speed)


def lookup(mineral_ids, values_table):
    kinds = jnp.arange(values_table.shape[0], dtype=jnp.int32)[:, None, None, None]
    return jnp.sum(jnp.where(mineral_ids[None] == kinds, values_table[:, None, None, None], 0.0), 0)


def pull_global(values, shift_z, shift_y, shift_x):
    rolled = jnp.roll(values, shift_z, axis=0)
    if shift_y == 1:
        rolled = jnp.concatenate([jnp.zeros_like(rolled[:, :1]), rolled[:, :-1]], 1)
    elif shift_y == -1:
        rolled = jnp.concatenate([rolled[:, 1:], jnp.zeros_like(rolled[:, :1])], 1)
    return jnp.roll(rolled, shift_x, axis=2)


def stream(relaxed, pore_mask, links_count):
    results = []
    for direction in range(links_count):
        shift_z, shift_y, shift_x = (int(v) for v in LINKS19[direction])
        source = pull_global(pore_mask, shift_z, shift_y, shift_x)
        arrived = pull_global(relaxed[direction], shift_z, shift_y, shift_x)
        results.append(jnp.where(source == 0, relaxed[REVERSE19[direction]], arrived))
    return jnp.stack(results)


def reference(populations, solute, pore_mask, mineral_ids, reaction_rates, saturation):
    density = jnp.sum(populations, 0)
    velocity = moment(populations, LINKS19) / density
    balanced = equilibrium(density, velocity, LINKS19, WEIGHTS19, 3.0, 4.5, 1.5)
    relaxed = populations - (populations - balanced) / RELAX_FLOW
    flow_next = jnp.where(pore_mask[None] == 0, populations, stream(relaxed, pore_mask, 19))
    density_next = jnp.sum(flow_next, 0)
    velocity_next = jnp.where(pore_mask[None] > 0, moment(flow_next, LINKS19) / density_next, 0.0)
    concentration = jnp.sum(solute, 0)
    rate_cell = lookup(mineral_ids, reaction_rates)
    target = lookup(mineral_ids, saturation)
    reaction = jnp.where(pore_mask == 2, -rate_cell * (concentration - target), 0.0)
    solute_balanced = equilibrium(concentration, velocity_next, LINKS19[:7], WEIGHTS7, 4.0, 0.0, 0.0)
    weights = jnp.asarray(WEIGHTS7, jnp.float32)[:, None, None, None]
    solute_relaxed = solute - (solute - solute_balanced) / RELAX_SOLUTE + weights * reaction
    solute_next = jnp.where(pore_mask[None] == 0, solute, stream(solute_relaxed, pore_mask, 7))
    return flow_next, solute_next
```

```python
import functools

import jax
import jax.numpy as jnp
import numpy as np
from jax import lax
from jax.experimental import pallas as pl
from jax.experimental.pallas import tpu as pltpu
from jax.sharding import PartitionSpec as P

LINKS19 = np.array(
    [
        [0, 0, 0],
        [1, 0, 0],
        [-1, 0, 0],
        [0, 1, 0],
        [0, -1, 0],
        [0, 0, 1],
        [0, 0, -1],
        [1, 1, 0],
        [-1, -1, 0],
        [1, -1, 0],
        [-1, 1, 0],
        [1, 0, 1],
        [-1, 0, -1],
        [1, 0, -1],
        [-1, 0, 1],
        [0, 1, 1],
        [0, -1, -1],
        [0, 1, -1],
        [0, -1, 1],
    ]
)
REVERSE19 = [0, 2, 1, 4, 3, 6, 5, 8, 7, 10, 9, 12, 11, 14, 13, 16, 15, 18, 17]
WEIGHTS19 = np.array([1.0 / 3.0] + [1.0 / 18.0] * 6 + [1.0 / 36.0] * 12)
WEIGHTS7 = np.array([0.25] + [0.125] * 6)
RELAX_FLOW = 1.25
RELAX_SOLUTE = 1.4


RISING = [d for d in range(19) if LINKS19[d][0] == 1]
FALLING = [d for d in range(19) if LINKS19[d][0] == -1]
ACROSS_UP = [d for d in range(19) if LINKS19[d][1] == 1]
ACROSS_DOWN = [d for d in range(19) if LINKS19[d][1] == -1]
CORNERS = [d for d in range(19) if LINKS19[d][0] != 0 and LINKS19[d][1] != 0]
TOP = 8
MESH = pl.DeviceIdType.MESH


def total(terms):
    terms = list(terms)
    while len(terms) > 1:
        terms = [sum(terms[i : i + 2][1:], terms[i]) for i in range(0, len(terms), 2)]
    return terms[0]


def momentum(values, axis):
    plus = total([values[d] for d in range(19) if LINKS19[d][axis] == 1])
    minus = total([values[d] for d in range(19) if LINKS19[d][axis] == -1])
    return plus - minus


def along(velocity, direction):
    parts = [(int(e), u) for e, u in zip(LINKS19[direction], velocity) if e != 0]
    sign, result = parts[0]
    result = result if sign == 1 else -result
    for sign, u in parts[1:]:
        result = result + u if sign == 1 else result - u
    return result


def kernel(
    pop_in, sol_in, mask_in, ids_in, rates, targets, flow_out, sol_out,
    pop, sol, mask, ids, relaxed, rock, carried,
    y_out, y_in, corner_out, corner_in, s_out, s_in,
    load_sem, store_sem, send_sem, recv_sem,
):
    _, depth, width, lanes = pop.shape
    last = depth - 1
    chunks = width // 8
    below_first, after_last = TOP - 1, TOP + width
    gz, gy = lax.axis_index("gz"), lax.axis_index("gy")
    nz, ny = lax.axis_size("gz"), lax.axis_size("gy")
    up, down = lax.rem(gz + 1, nz), lax.rem(gz + nz - 1, nz)
    right, left = lax.rem(gy + 1, ny), lax.rem(gy + ny - 1, ny)
    to_z = {1: up, 0: gz, -1: down}
    to_y = {1: right, 0: gy, -1: left}

    loads = [pltpu.make_async_copy(mask_in, mask, load_sem.at[0])]
    order = [0, last] + list(range(1, last))
    for k, p in enumerate(order):
        loads.append(
            pltpu.make_async_copy(pop_in.at[:, p], pop.at[:, p], load_sem.at[1 + k])
        )
    loads.append(pltpu.make_async_copy(sol_in, sol, load_sem.at[1 + depth]))
    loads.append(pltpu.make_async_copy(ids_in, ids, load_sem.at[2 + depth]))
    for copy in loads:
        copy.start()

    barrier = pltpu.get_barrier_semaphore()
    for ez in (1, 0, -1):
        for ey in (1, 0, -1):
            if (ez, ey) != (0, 0):
                pl.semaphore_signal(
                    barrier, inc=1, device_id=(to_z[ez], to_y[ey]), device_id_type=MESH
                )

    def remote(source, target, slot, ez, ey):
        return pltpu.make_async_remote_copy(
            src_ref=source,
            dst_ref=target,
            send_sem=send_sem.at[slot],
            recv_sem=recv_sem.at[slot],
            device_id=(to_z[ez], to_y[ey]),
            device_id_type=MESH,
        )

    inner = pl.ds(TOP, width)

    loads[0].wait()
    for p in range(depth):
        rock[p + 1, TOP : TOP + width] = mask[p].astype(jnp.float32)

    def relax(p):
        def step(c, _):
            rows = pl.ds(pl.multiple_of(c * 8, 8), 8)
            spread = pl.ds(pl.multiple_of(c * 8 + TOP, 8), 8)
            f = [pop[d, p, rows] for d in range(19)]
            density = total(f)
            inverse = 1.0 / density
            velocity = [momentum(f, axis) * inverse for axis in range(3)]
            speed = total([u * u for u in velocity])
            share = 1.0 / RELAX_FLOW
            rest = 1.0 - 1.5 * speed
            scaled = {w: density * float(share * w) for w in sorted(set(WEIGHTS19))}
            relaxed[0, p + 1, spread] = (1.0 - share) * f[0] + scaled[WEIGHTS19[0]] * rest
            for d in range(1, 19, 2):
                projected = along(velocity, d)
                even = rest + 4.5 * projected * projected
                odd = 3.0 * projected
                weight = scaled[WEIGHTS19[d]]
                relaxed[d, p + 1, spread] = (1.0 - share) * f[d] + weight * (even + odd)
                relaxed[d + 1, p + 1, spread] = (1.0 - share) * f[d + 1] + weight * (even - odd)
            return 0

        lax.fori_loop(0, chunks, step, 0)

    loads[1].wait()
    relax(0)
    loads[2].wait()
    relax(last)
    first_row, end_row = TOP, TOP + width - 1
    for k, d in enumerate(CORNERS):
        p = depth if LINKS19[d][0] == 1 else 1
        r = end_row if LINKS19[d][1] == 1 else first_row
        corner_out[k, 0:1] = relaxed[d, p, r : r + 1]
        corner_out[k, 1:2] = rock[p, r : r + 1]

    pl.semaphore_wait(barrier, 8)
    to_up = [remote(rock.at[depth, inner], rock.at[0, inner], 0, 1, 0)]
    to_down = [remote(rock.at[1, inner], rock.at[depth + 1, inner], 1, -1, 0)]
    for k, (d, e) in enumerate(zip(RISING, FALLING)):
        to_up.append(
            remote(relaxed.at[d, depth, inner], relaxed.at[d, 0, inner], 2 + 2 * k, 1, 0)
        )
        to_down.append(
            remote(relaxed.at[e, 1, inner], relaxed.at[e, depth + 1, inner], 3 + 2 * k, -1, 0)
        )
    corners = [
        remote(
            corner_out.at[k], corner_in.at[k], 12 + k, int(LINKS19[d][0]), int(LINKS19[d][1])
        )
        for k, d in enumerate(CORNERS)
    ]
    for copy in corners:
        copy.start()
    for a, b in zip(to_up, to_down):
        a.start()
        b.start()

    for k in range(2, depth):
        loads[1 + k].wait()
    lax.fori_loop(1, last, lambda p, _: (relax(p), 0)[1], 0)
    for side, links, r in ((0, ACROSS_UP, end_row), (1, ACROSS_DOWN, first_row)):
        for k, d in enumerate(links):
            for p in range(depth):
                row = k * depth + p
                y_out[side, row : row + 1] = relaxed[d, p + 1, r : r + 1]
        for p in range(depth):
            row = 5 * depth + p
            y_out[side, row : row + 1] = rock[p + 1, r : r + 1]
    y_copies = [
        remote(y_out.at[0], y_in.at[0], 16, 0, 1),
        remote(y_out.at[1], y_in.at[1], 17, 0, -1),
    ]
    for copy in y_copies:
        copy.start()
    loads[1 + depth].wait()
    loads[2 + depth].wait()
    for copy in y_copies:
        copy.wait_recv()
    open_side = [
        jnp.where(gy == 0, 0.0, 1.0),
        jnp.where(gy == ny - 1, 0.0, 1.0),
    ]
    for side, links, r in ((0, ACROSS_UP, below_first), (1, ACROSS_DOWN, after_last)):
        for k, d in enumerate(links):
            for p in range(depth):
                row = k * depth + p
                relaxed[d, p + 1, r : r + 1] = y_in[side, row : row + 1]
        for p in range(depth):
            row = 5 * depth + p
            rock[p + 1, r : r + 1] = y_in[side, row : row + 1] * open_side[side]

    def source_rock(direction, p, c):
        ez, ey, ex = (int(v) for v in LINKS19[direction])
        found = rock[p + 1 - ez, pl.ds(TOP - ey + c * 8, 8)]
        return found if ex == 0 else pltpu.roll(found, ex % lanes, 1)

    def pulled(store, direction, p, c):
        ez, ey, ex = (int(v) for v in LINKS19[direction])
        found = store[direction, p + 1 - ez, pl.ds(TOP - ey + c * 8, 8)]
        return found if ex == 0 else pltpu.roll(found, ex % lanes, 1)

    def flow_rows(p, c):
        rows = pl.ds(c * 8, 8)
        spread = pl.ds(c * 8 + TOP, 8)
        here = mask[p, rows]
        solid = here == 0
        flow = []
        for d in range(19):
            if d == 0:
                passed = relaxed[0, p + 1, spread]
            else:
                passed = jnp.where(
                    source_rock(d, p, c) == 0.0,
                    relaxed[REVERSE19[d], p + 1, spread],
                    pulled(relaxed, d, p, c),
                )
            value = jnp.where(solid, pop[d, p, rows], passed)
            pop[d, p, rows] = value
            flow.append(value)
        inverse = jnp.where(solid, 0.0, 1.0 / total(flow))
        velocity = [momentum(flow, axis) * inverse for axis in range(3)]
        s = [sol[d, p, rows] for d in range(7)]
        concentration = total(s)
        kind = ids[p, rows]
        rate = jnp.zeros_like(concentration)
        target = jnp.zeros_like(concentration)
        for k in range(rates.shape[0]):
            chosen = kind == k
            rate = jnp.where(chosen, rates[k], rate)
            target = jnp.where(chosen, targets[k], target)
        reaction = jnp.where(here == 2, rate * (target - concentration), 0.0)
        share = 1.0 / RELAX_SOLUTE
        for weight, links in ((0.25, (0,)), (0.125, range(1, 7))):
            level = weight * (share * concentration + reaction)
            slope = (4.0 * share * weight) * concentration
            for d in links:
                value = (1.0 - share) * s[d] + level
                if d:
                    value = value + slope * along(velocity, d)
                carried[d, p + 1, spread] = value

    def solute_rows(p, c):
        rows = pl.ds(c * 8, 8)
        spread = pl.ds(c * 8 + TOP, 8)
        solid = mask[p, rows] == 0
        for d in range(7):
            if d == 0:
                passed = carried[0, p + 1, spread]
            else:
                passed = jnp.where(
                    source_rock(d, p, c) == 0.0,
                    carried[REVERSE19[d], p + 1, spread],
                    pulled(carried, d, p, c),
                )
            sol[d, p, rows] = jnp.where(solid, sol[d, p, rows], passed)

    def plane(rows_of, p):
        for c in range(chunks):
            rows_of(p, c)

    stores = []

    def store(source, target, p):
        copy = pltpu.make_async_copy(source.at[:, p], target.at[:, p], store_sem.at[len(stores)])
        copy.start()
        stores.append(copy)

    lax.fori_loop(1, last, lambda p, _: (plane(flow_rows, p), 0)[1], 0)
    for p in range(1, last):
        store(pop, flow_out, p)

    for copy in corners:
        copy.wait_recv()
    for k, d in enumerate(CORNERS):
        p = 0 if LINKS19[d][0] == 1 else depth + 1
        side, r = (0, below_first) if LINKS19[d][1] == 1 else (1, after_last)
        relaxed[d, p, r : r + 1] = corner_in[k, 0:1]
        rock[p, r : r + 1] = corner_in[k, 1:2] * open_side[side]

    s_up = remote(carried.at[1, depth, inner], carried.at[1, 0, inner], 18, 1, 0)
    s_down = remote(carried.at[2, 1, inner], carried.at[2, depth + 1, inner], 19, -1, 0)
    for copy in to_up:
        copy.wait_recv()
    plane(flow_rows, 0)
    s_down.start()
    store(pop, flow_out, 0)
    for copy in to_down:
        copy.wait_recv()
    plane(flow_rows, last)
    s_up.start()
    store(pop, flow_out, last)

    for side, d, r in ((0, 3, end_row), (1, 4, first_row)):
        for p in range(depth):
            s_out[side, p : p + 1] = carried[d, p + 1, r : r + 1]
    s_copies = [
        remote(s_out.at[0], s_in.at[0], 20, 0, 1),
        remote(s_out.at[1], s_in.at[1], 21, 0, -1),
    ]
    for copy in s_copies:
        copy.start()
    for copy in s_copies:
        copy.wait_recv()
    for side, d, r in ((0, 3, below_first), (1, 4, after_last)):
        for p in range(depth):
            carried[d, p + 1, r : r + 1] = s_in[side, p : p + 1]
    lax.fori_loop(1, last, lambda p, _: (plane(solute_rows, p), 0)[1], 0)
    for p in range(1, last):
        store(sol, sol_out, p)
    s_up.wait_recv()
    plane(solute_rows, 0)
    store(sol, sol_out, 0)
    s_down.wait_recv()
    plane(solute_rows, last)
    store(sol, sol_out, last)

    for copy in to_up + to_down + corners + y_copies + s_copies + [s_up, s_down]:
        copy.wait_send()
    for copy in stores:
        copy.wait()


def on_device(populations, solute, pore_mask, mineral_ids, reaction_rates, saturation):
    depth, width, lanes = pore_mask.shape
    rows = TOP + width + 8
    f32 = jnp.float32
    y_rows = -(-6 * depth // 8) * 8
    s_rows = -(-depth // 8) * 8
    anywhere = pl.BlockSpec(memory_space=pl.ANY)
    scalars = pl.BlockSpec(memory_space=pltpu.SMEM)
    return tuple(
        pl.pallas_call(
            kernel,
            out_shape=(
                jax.ShapeDtypeStruct(populations.shape, f32),
                jax.ShapeDtypeStruct(solute.shape, f32),
            ),
            in_specs=[anywhere] * 4 + [scalars] * 2,
            out_specs=(anywhere, anywhere),
            scratch_shapes=[
                pltpu.VMEM(populations.shape, f32),
                pltpu.VMEM(solute.shape, f32),
                pltpu.VMEM(pore_mask.shape, jnp.int32),
                pltpu.VMEM(mineral_ids.shape, jnp.int32),
                pltpu.VMEM((19, depth + 2, rows, lanes), f32),
                pltpu.VMEM((depth + 2, rows, lanes), f32),
                pltpu.VMEM((7, depth + 2, rows, lanes), f32),
                pltpu.VMEM((2, y_rows, lanes), f32),
                pltpu.VMEM((2, y_rows, lanes), f32),
                pltpu.VMEM((4, 8, lanes), f32),
                pltpu.VMEM((4, 8, lanes), f32),
                pltpu.VMEM((2, s_rows, lanes), f32),
                pltpu.VMEM((2, s_rows, lanes), f32),
                pltpu.SemaphoreType.DMA((depth + 3,)),
                pltpu.SemaphoreType.DMA((2 * depth,)),
                pltpu.SemaphoreType.DMA((22,)),
                pltpu.SemaphoreType.DMA((22,)),
            ],
            compiler_params=pltpu.CompilerParams(collective_id=0, has_side_effects=True),
        )(populations, solute, pore_mask, mineral_ids, reaction_rates, saturation)
    )


def solution(mesh):
    return jax.shard_map(
        on_device,
        mesh=mesh,
        in_specs=(
            P(None, "gz", "gy", None),
            P(None, "gz", "gy", None),
            P("gz", "gy", None),
            P("gz", "gy", None),
            P(),
            P(),
        ),
        out_specs=(P(None, "gz", "gy", None), P(None, "gz", "gy", None)),
        check_vma=False,
    )
```

```python
import functools

import jax
import jax.numpy as jnp
import numpy as np
from jax import lax
from jax.experimental import pallas as pl
from jax.experimental.pallas import tpu as pltpu
from jax.sharding import PartitionSpec as P

LINKS19 = np.array(
    [
        [0, 0, 0],
        [1, 0, 0],
        [-1, 0, 0],
        [0, 1, 0],
        [0, -1, 0],
        [0, 0, 1],
        [0, 0, -1],
        [1, 1, 0],
        [-1, -1, 0],
        [1, -1, 0],
        [-1, 1, 0],
        [1, 0, 1],
        [-1, 0, -1],
        [1, 0, -1],
        [-1, 0, 1],
        [0, 1, 1],
        [0, -1, -1],
        [0, 1, -1],
        [0, -1, 1],
    ]
)
REVERSE19 = [0, 2, 1, 4, 3, 6, 5, 8, 7, 10, 9, 12, 11, 14, 13, 16, 15, 18, 17]
WEIGHTS19 = np.array([1.0 / 3.0] + [1.0 / 18.0] * 6 + [1.0 / 36.0] * 12)
WEIGHTS7 = np.array([0.25] + [0.125] * 6)
RELAX_FLOW = 1.25
RELAX_SOLUTE = 1.4


RISING = [d for d in range(19) if LINKS19[d][0] == 1]
FALLING = [d for d in range(19) if LINKS19[d][0] == -1]
ACROSS_UP = [d for d in range(19) if LINKS19[d][1] == 1]
ACROSS_DOWN = [d for d in range(19) if LINKS19[d][1] == -1]
CORNERS = [d for d in range(19) if LINKS19[d][0] != 0 and LINKS19[d][1] != 0]
TOP = 8
MESH = pl.DeviceIdType.MESH


def total(terms):
    terms = list(terms)
    while len(terms) > 1:
        terms = [sum(terms[i : i + 2][1:], terms[i]) for i in range(0, len(terms), 2)]
    return terms[0]


def momentum(values, axis):
    plus = total([values[d] for d in range(19) if LINKS19[d][axis] == 1])
    minus = total([values[d] for d in range(19) if LINKS19[d][axis] == -1])
    return plus - minus


def along(velocity, direction):
    parts = [(int(e), u) for e, u in zip(LINKS19[direction], velocity) if e != 0]
    sign, result = parts[0]
    result = result if sign == 1 else -result
    for sign, u in parts[1:]:
        result = result + u if sign == 1 else result - u
    return result


def source_rock(rock, direction, p, c):
    ez, ey, ex = (int(v) for v in LINKS19[direction])
    found = rock[p + 1 - ez, pl.ds(TOP - ey + c * 8, 8)]
    return found if ex == 0 else pltpu.roll(found, ex % rock.shape[-1], 1)


def pulled(store, direction, p, c):
    ez, ey, ex = (int(v) for v in LINKS19[direction])
    found = store[direction, p + 1 - ez, pl.ds(TOP - ey + c * 8, 8)]
    return found if ex == 0 else pltpu.roll(found, ex % store.shape[-1], 1)


def kernel(
    pop_in, sol_in, mask_in, ids_in, rates, targets,
    pop, sol, carried, rock, mask, ids, relaxed,
    y_out, y_in, corner_out, corner_in, s_out, s_in,
    load_sem, send_sem, recv_sem,
):
    _, depth, width, lanes = pop.shape
    last = depth - 1
    chunks = width // 8
    below_first, after_last = TOP - 1, TOP + width
    gz, gy = lax.axis_index("gz"), lax.axis_index("gy")
    nz, ny = lax.axis_size("gz"), lax.axis_size("gy")
    up, down = lax.rem(gz + 1, nz), lax.rem(gz + nz - 1, nz)
    right, left = lax.rem(gy + 1, ny), lax.rem(gy + ny - 1, ny)
    to_z = {1: up, 0: gz, -1: down}
    to_y = {1: right, 0: gy, -1: left}

    loads = [pltpu.make_async_copy(mask_in, mask, load_sem.at[0])]
    order = [0, last] + list(range(1, last))
    for k, p in enumerate(order):
        loads.append(
            pltpu.make_async_copy(pop_in.at[:, p], pop.at[:, p], load_sem.at[1 + k])
        )
    loads.append(pltpu.make_async_copy(sol_in, sol, load_sem.at[1 + depth]))
    loads.append(pltpu.make_async_copy(ids_in, ids, load_sem.at[2 + depth]))
    for copy in loads:
        copy.start()

    barrier = pltpu.get_barrier_semaphore()
    for ez in (1, 0, -1):
        for ey in (1, 0, -1):
            if (ez, ey) != (0, 0):
                pl.semaphore_signal(
                    barrier, inc=1, device_id=(to_z[ez], to_y[ey]), device_id_type=MESH
                )

    def remote(source, target, slot, ez, ey):
        return pltpu.make_async_remote_copy(
            src_ref=source,
            dst_ref=target,
            send_sem=send_sem.at[slot],
            recv_sem=recv_sem.at[slot],
            device_id=(to_z[ez], to_y[ey]),
            device_id_type=MESH,
        )

    inner = pl.ds(TOP, width)

    loads[0].wait()
    for p in range(depth):
        rock[p + 1, TOP : TOP + width] = mask[p].astype(jnp.float32)

    def relax(p):
        def step(c, _):
            rows = pl.ds(pl.multiple_of(c * 8, 8), 8)
            spread = pl.ds(pl.multiple_of(c * 8 + TOP, 8), 8)
            f = [pop[d, p, rows] for d in range(19)]
            density = total(f)
            inverse = 1.0 / density
            velocity = [momentum(f, axis) * inverse for axis in range(3)]
            speed = total([u * u for u in velocity])
            share = 1.0 / RELAX_FLOW
            rest = 1.0 - 1.5 * speed
            scaled = {w: density * float(share * w) for w in sorted(set(WEIGHTS19))}
            relaxed[0, p + 1, spread] = (1.0 - share) * f[0] + scaled[WEIGHTS19[0]] * rest
            for d in range(1, 19, 2):
                projected = along(velocity, d)
                even = rest + 4.5 * projected * projected
                odd = 3.0 * projected
                weight = scaled[WEIGHTS19[d]]
                relaxed[d, p + 1, spread] = (1.0 - share) * f[d] + weight * (even + odd)
                relaxed[d + 1, p + 1, spread] = (1.0 - share) * f[d + 1] + weight * (even - odd)
            return 0

        lax.fori_loop(0, chunks, step, 0)

    loads[1].wait()
    relax(0)
    loads[2].wait()
    relax(last)
    first_row, end_row = TOP, TOP + width - 1
    for k, d in enumerate(CORNERS):
        p = depth if LINKS19[d][0] == 1 else 1
        r = end_row if LINKS19[d][1] == 1 else first_row
        corner_out[k, 0:1] = relaxed[d, p, r : r + 1]
        corner_out[k, 1:2] = rock[p, r : r + 1]

    pl.semaphore_wait(barrier, 8)
    to_up = [remote(rock.at[depth, inner], rock.at[0, inner], 0, 1, 0)]
    to_down = [remote(rock.at[1, inner], rock.at[depth + 1, inner], 1, -1, 0)]
    for k, (d, e) in enumerate(zip(RISING, FALLING)):
        to_up.append(
            remote(relaxed.at[d, depth, inner], relaxed.at[d, 0, inner], 2 + 2 * k, 1, 0)
        )
        to_down.append(
            remote(relaxed.at[e, 1, inner], relaxed.at[e, depth + 1, inner], 3 + 2 * k, -1, 0)
        )
    corners = [
        remote(
            corner_out.at[k], corner_in.at[k], 12 + k, int(LINKS19[d][0]), int(LINKS19[d][1])
        )
        for k, d in enumerate(CORNERS)
    ]
    for copy in corners:
        copy.start()
    for a, b in zip(to_up, to_down):
        a.start()
        b.start()

    for k in range(2, depth):
        loads[1 + k].wait()
    lax.fori_loop(1, last, lambda p, _: (relax(p), 0)[1], 0)
    for side, links, r in ((0, ACROSS_UP, end_row), (1, ACROSS_DOWN, first_row)):
        for k, d in enumerate(links):
            for p in range(depth):
                row = k * depth + p
                y_out[side, row : row + 1] = relaxed[d, p + 1, r : r + 1]
        for p in range(depth):
            row = 5 * depth + p
            y_out[side, row : row + 1] = rock[p + 1, r : r + 1]
    y_copies = [
        remote(y_out.at[0], y_in.at[0], 16, 0, 1),
        remote(y_out.at[1], y_in.at[1], 17, 0, -1),
    ]
    for copy in y_copies:
        copy.start()
    loads[1 + depth].wait()
    loads[2 + depth].wait()
    for copy in y_copies:
        copy.wait_recv()
    open_side = [
        jnp.where(gy == 0, 0.0, 1.0),
        jnp.where(gy == ny - 1, 0.0, 1.0),
    ]
    for side, links, r in ((0, ACROSS_UP, below_first), (1, ACROSS_DOWN, after_last)):
        for k, d in enumerate(links):
            for p in range(depth):
                row = k * depth + p
                relaxed[d, p + 1, r : r + 1] = y_in[side, row : row + 1]
        for p in range(depth):
            row = 5 * depth + p
            rock[p + 1, r : r + 1] = y_in[side, row : row + 1] * open_side[side]

    def flow_rows(p, c):
        rows = pl.ds(c * 8, 8)
        spread = pl.ds(c * 8 + TOP, 8)
        here = mask[p, rows]
        solid = here == 0
        flow = []
        for d in range(19):
            if d == 0:
                passed = relaxed[0, p + 1, spread]
            else:
                passed = jnp.where(
                    source_rock(rock, d, p, c) == 0.0,
                    relaxed[REVERSE19[d], p + 1, spread],
                    pulled(relaxed, d, p, c),
                )
            value = jnp.where(solid, pop[d, p, rows], passed)
            pop[d, p, rows] = value
            flow.append(value)
        inverse = jnp.where(solid, 0.0, 1.0 / total(flow))
        velocity = [momentum(flow, axis) * inverse for axis in range(3)]
        s = [sol[d, p, rows] for d in range(7)]
        concentration = total(s)
        kind = ids[p, rows]
        rate = jnp.zeros_like(concentration)
        target = jnp.zeros_like(concentration)
        for k in range(rates.shape[0]):
            chosen = kind == k
            rate = jnp.where(chosen, rates[k], rate)
            target = jnp.where(chosen, targets[k], target)
        reaction = jnp.where(here == 2, rate * (target - concentration), 0.0)
        share = 1.0 / RELAX_SOLUTE
        for weight, links in ((0.25, (0,)), (0.125, range(1, 7))):
            level = weight * (share * concentration + reaction)
            slope = (4.0 * share * weight) * concentration
            for d in links:
                value = (1.0 - share) * s[d] + level
                if d:
                    value = value + slope * along(velocity, d)
                carried[d, p + 1, spread] = value

    def plane(p):
        for c in range(chunks):
            flow_rows(p, c)

    lax.fori_loop(1, last, lambda p, _: (plane(p), 0)[1], 0)

    for copy in corners:
        copy.wait_recv()
    for k, d in enumerate(CORNERS):
        p = 0 if LINKS19[d][0] == 1 else depth + 1
        side, r = (0, below_first) if LINKS19[d][1] == 1 else (1, after_last)
        relaxed[d, p, r : r + 1] = corner_in[k, 0:1]
        rock[p, r : r + 1] = corner_in[k, 1:2] * open_side[side]

    s_up = remote(carried.at[1, depth, inner], carried.at[1, 0, inner], 18, 1, 0)
    s_down = remote(carried.at[2, 1, inner], carried.at[2, depth + 1, inner], 19, -1, 0)
    for copy in to_up:
        copy.wait_recv()
    plane(0)
    s_down.start()
    for copy in to_down:
        copy.wait_recv()
    plane(last)
    s_up.start()

    for side, d, r in ((0, 3, end_row), (1, 4, first_row)):
        for p in range(depth):
            s_out[side, p : p + 1] = carried[d, p + 1, r : r + 1]
    s_copies = [
        remote(s_out.at[0], s_in.at[0], 20, 0, 1),
        remote(s_out.at[1], s_in.at[1], 21, 0, -1),
    ]
    for copy in s_copies:
        copy.start()
    for copy in s_copies:
        copy.wait_recv()
    for side, d, r in ((0, 3, below_first), (1, 4, after_last)):
        for p in range(depth):
            carried[d, p + 1, r : r + 1] = s_in[side, p : p + 1]
    s_up.wait_recv()
    s_down.wait_recv()
    for copy in to_up + to_down + corners + y_copies + s_copies + [s_up, s_down]:
        copy.wait_send()


def finish(flow, sol, carried, rock, flow_out, sol_out, moved, store_sem):
    _, depth, width, lanes = sol.shape
    stores = [pltpu.make_async_copy(flow, flow_out, store_sem.at[0])]
    stores[0].start()

    for p in range(depth):
        for c in range(width // 8):
            rows = pl.ds(c * 8, 8)
            spread = pl.ds(c * 8 + TOP, 8)
            solid = rock[p + 1, spread] == 0.0
            for d in range(7):
                if d == 0:
                    passed = carried[0, p + 1, spread]
                else:
                    passed = jnp.where(
                        source_rock(rock, d, p, c) == 0.0,
                        carried[REVERSE19[d], p + 1, spread],
                        pulled(carried, d, p, c),
                    )
                moved[d, p, rows] = jnp.where(solid, sol[d, p, rows], passed)
        stores.append(
            pltpu.make_async_copy(moved.at[:, p], sol_out.at[:, p], store_sem.at[1 + p])
        )
        stores[-1].start()
    for copy in stores:
        copy.wait()


def on_device(populations, solute, pore_mask, mineral_ids, reaction_rates, saturation):
    depth, width, lanes = pore_mask.shape
    rows = TOP + width + 8
    f32 = jnp.float32
    y_rows = -(-6 * depth // 8) * 8
    s_rows = -(-depth // 8) * 8
    anywhere = pl.BlockSpec(memory_space=pltpu.HBM)
    scalars = pl.BlockSpec(memory_space=pltpu.SMEM)
    inside = pl.BlockSpec(memory_space=pltpu.VMEM)
    held = pl.pallas_call(
        kernel,
        out_shape=(
            pltpu.VMEM(populations.shape, f32),
            pltpu.VMEM(solute.shape, f32),
            pltpu.VMEM((7, depth + 2, rows, lanes), f32),
            pltpu.VMEM((depth + 2, rows, lanes), f32),
        ),
        in_specs=[anywhere] * 4 + [scalars] * 2,
        out_specs=(inside,) * 4,
        scratch_shapes=[
            pltpu.VMEM(pore_mask.shape, jnp.int32),
            pltpu.VMEM(mineral_ids.shape, jnp.int32),
            pltpu.VMEM((19, depth + 2, rows, lanes), f32),
            pltpu.VMEM((2, y_rows, lanes), f32),
            pltpu.VMEM((2, y_rows, lanes), f32),
            pltpu.VMEM((4, 8, lanes), f32),
            pltpu.VMEM((4, 8, lanes), f32),
            pltpu.VMEM((2, s_rows, lanes), f32),
            pltpu.VMEM((2, s_rows, lanes), f32),
            pltpu.SemaphoreType.DMA((depth + 3,)),
            pltpu.SemaphoreType.DMA((22,)),
            pltpu.SemaphoreType.DMA((22,)),
        ],
        compiler_params=pltpu.CompilerParams(
            collective_id=0, has_side_effects=True, vmem_limit_bytes=24 * 2**20
        ),
    )(populations, solute, pore_mask, mineral_ids, reaction_rates, saturation)
    return tuple(
        pl.pallas_call(
            finish,
            out_shape=(
                jax.ShapeDtypeStruct(populations.shape, f32),
                jax.ShapeDtypeStruct(solute.shape, f32),
            ),
            in_specs=[inside] * 4,
            out_specs=(anywhere, anywhere),
            scratch_shapes=[
                pltpu.VMEM(solute.shape, f32),
                pltpu.SemaphoreType.DMA((depth + 1,)),
            ],
            compiler_params=pltpu.CompilerParams(vmem_limit_bytes=24 * 2**20),
        )(*held)
    )


def solution(mesh):
    return jax.shard_map(
        on_device,
        mesh=mesh,
        in_specs=(
            P(None, "gz", "gy", None),
            P(None, "gz", "gy", None),
            P("gz", "gy", None),
            P("gz", "gy", None),
            P(),
            P(),
        ),
        out_specs=(P(None, "gz", "gy", None), P(None, "gz", "gy", None)),
        check_vma=False,
    )
```
